8 devices in a mesh: dp: 1 (over z), tp: 8 (over y, x, core).
Axes of the slice: x: 2, y: 2, z: 1, core: 2. Of those that a mesh axis runs over, the one named last changes fastest.
Arguments:
- tokens: int32 [4], P('dp')
- lengths: int32 [4], P('dp')
- embed_table: bfloat16 [49152, 3840], P('tp')
- norm_gains: bfloat16 [9, 3840], replicated
- w_query: bfloat16 [2, 3840, 4096], P(None, None, 'tp')
- w_key: bfloat16 [2, 3840, 2048], P(None, None, 'tp')
- w_value: bfloat16 [2, 3840, 2048], P(None, None, 'tp')
- w_out: bfloat16 [2, 4096, 3840], P(None, 'tp')
- w_gate: bfloat16 [2, 3840, 15360], P(None, None, 'tp')
- w_up: bfloat16 [2, 3840, 15360], P(None, None, 'tp')
- w_down: bfloat16 [2, 15360, 3840], P(None, 'tp')
- key_local: bfloat16 [4, 1024, 8, 256], P('dp', None, 'tp')
- value_local: bfloat16 [4, 1024, 8, 256], P('dp', None, 'tp')
- key_global: bfloat16 [4, 4096, 8, 256], P('dp', None, 'tp')
- value_global: bfloat16 [4, 4096, 8, 256], P('dp', None, 'tp')
Outputs:
- output 1: float32 [4, 49152], P('dp', 'tp')
- output 2: bfloat16 [2, 4, 2048], P(None, 'dp', 'tp')
- output 3: bfloat16 [2, 4, 2048], P(None, 'dp', 'tp')
All inputs are finite; a program needn't handle non-finite values.
Results may differ from the reference program's by a relative error of at most 0.02.
Values are sent between devices in bfloat16 or wider.
A program may use at most 1 GiB of HBM per device.

```python
import math
import jax
import jax.numpy as jnp
from jax import lax

MODEL_DIM = 3840
Q_HEADS = 16
KV_HEADS = 8
HEAD_DIM = 256
FF_DIM = 15360
WINDOW = 1024
VOCAB_SIZE = 49152
CACHE_LEN = 4096
BATCH_PART = 4


def setup_inputs(seed: int = 0, part: int = 0) -> dict:
    base_key = jax.random.key(seed)
    shared_keys = jax.random.split(base_key, 10)
    part_keys = jax.random.split(jax.random.fold_in(base_key, part), 6)
    q_width = Q_HEADS * HEAD_DIM
    kv_width = KV_HEADS * HEAD_DIM

    def normal_bf16(rng_key, shape, std_dev):
        return (jax.random.normal(rng_key, shape, jnp.float32) * std_dev).astype(jnp.bfloat16)

    tokens = jax.random.randint(part_keys[0], (BATCH_PART,), 0, VOCAB_SIZE, dtype=jnp.int32)
    lengths = jax.random.randint(part_keys[1], (BATCH_PART,), 0, CACHE_LEN, dtype=jnp.int32)
    lengths = lengths.at[BATCH_PART - 1].set(lengths[BATCH_PART - 1] % WINDOW)
    lengths = lengths.at[0].set(CACHE_LEN - 1)
    local_shape = (BATCH_PART, WINDOW, KV_HEADS, HEAD_DIM)
    global_shape = (BATCH_PART, CACHE_LEN, KV_HEADS, HEAD_DIM)
    return {
        "tokens": tokens,
        "lengths": lengths,
        "embed_table": normal_bf16(shared_keys[0], (VOCAB_SIZE, MODEL_DIM), MODEL_DIM ** -0.5),
        "norm_gains": normal_bf16(shared_keys[1], (9, MODEL_DIM), 0.3),
        "w_query": normal_bf16(shared_keys[2], (2, MODEL_DIM, q_width), MODEL_DIM ** -0.5),
        "w_key": normal_bf16(shared_keys[3], (2, MODEL_DIM, kv_width), MODEL_DIM ** -0.5),
        "w_value": normal_bf16(shared_keys[4], (2, MODEL_DIM, kv_width), MODEL_DIM ** -0.5),
        "w_out": normal_bf16(shared_keys[5], (2, q_width, MODEL_DIM), q_width ** -0.5),
        "w_gate": normal_bf16(shared_keys[6], (2, MODEL_DIM, FF_DIM), MODEL_DIM ** -0.5),
        "w_up": normal_bf16(shared_keys[7], (2, MODEL_DIM, FF_DIM), MODEL_DIM ** -0.5),
        "w_down": normal_bf16(shared_keys[8], (2, FF_DIM, MODEL_DIM), FF_DIM ** -0.5),
        "key_local": normal_bf16(part_keys[2], local_shape, 1.0),
        "value_local": normal_bf16(part_keys[3], local_shape, 1.0),
        "key_global": normal_bf16(part_keys[4], global_shape, 1.0),
        "value_global": normal_bf16(part_keys[5], global_shape, 1.0),
    }


def rms_norm(hidden, gain):
    values = hidden.astype(jnp.float32)
    inv_rms = lax.rsqrt(jnp.mean(values * values, axis=-1, keepdims=True) + 1e-6)
    return (values * inv_rms * (1.0 + gain.astype(jnp.float32))).astype(jnp.bfloat16)


def rope_rotate(heads, lengths):
    half_dim = HEAD_DIM // 2
    inv_freq = 10000.0 ** (-2.0 * jnp.arange(half_dim, dtype=jnp.float32) / HEAD_DIM)
    angles = lengths.astype(jnp.float32)[:, None, None] * inv_freq
    cos_tab = jnp.cos(angles)
    sin_tab = jnp.sin(angles)
    lower_half = heads[..., :half_dim].astype(jnp.float32)
    upper_half = heads[..., half_dim:].astype(jnp.float32)
    return jnp.concatenate([lower_half * cos_tab - upper_half * sin_tab, upper_half * cos_tab + lower_half * sin_tab], axis=-1)


def attend_request(queries, key_cache, value_cache, length, is_local):
    groups = Q_HEADS // KV_HEADS
    slots_total = key_cache.shape[0]
    grouped = queries.astype(jnp.float32).reshape(KV_HEADS, groups, HEAD_DIM)
    scores = jnp.einsum("kgd,skd->kgs", grouped, key_cache.astype(jnp.float32))
    capped = 50.0 * jnp.tanh(scores / 50.0)
    slot_ids = jnp.arange(slots_total, dtype=jnp.int32)
    valid_slots = slot_ids <= length
    if is_local:
        valid_slots = valid_slots | (length >= slots_total - 1)
    capped = jnp.where(valid_slots, capped, -1e30)
    attn_probs = jax.nn.softmax(capped, axis=-1).astype(jnp.bfloat16)
    attn_mixed = jnp.einsum("kgs,skd->kgd", attn_probs.astype(jnp.float32), value_cache.astype(jnp.float32))
    return attn_mixed.astype(jnp.bfloat16).reshape(Q_HEADS * HEAD_DIM)


def project(normed, weight):
    return jnp.dot(normed, weight, preferred_element_type=jnp.float32).astype(jnp.bfloat16)


def decoder_layer(hidden, lengths, layer_gains, w_query, w_key, w_value, w_out, w_gate, w_up, w_down, key_cache, value_cache, is_local):
    batch_size = hidden.shape[0]
    normed = rms_norm(hidden, layer_gains[0])
    queries = project(normed, w_query).reshape(batch_size, Q_HEADS, HEAD_DIM)
    new_keys = project(normed, w_key).reshape(batch_size, KV_HEADS, HEAD_DIM)
    new_values = project(normed, w_value).reshape(batch_size, KV_HEADS, HEAD_DIM)
    queries = (rope_rotate(queries, lengths) * 0.0625).astype(jnp.bfloat16)
    new_keys = rope_rotate(new_keys, lengths).astype(jnp.bfloat16)
    write_slots = lengths % WINDOW if is_local else lengths
    request_ids = jnp.arange(batch_size)
    key_cache = key_cache.at[request_ids, write_slots].set(new_keys)
    value_cache = value_cache.at[request_ids, write_slots].set(new_values)
    attn_mixed = lax.map(lambda request: attend_request(request[0], request[1], request[2], request[3], is_local), (queries, key_cache, value_cache, lengths))
    attn_out = project(attn_mixed, w_out)
    hidden = (hidden.astype(jnp.float32) + rms_norm(attn_out, layer_gains[1]).astype(jnp.float32)).astype(jnp.bfloat16)
    normed = rms_norm(hidden, layer_gains[2])
    gate_proj = project(normed, w_gate)
    up_proj = project(normed, w_up)
    activated = (jax.nn.gelu(gate_proj.astype(jnp.float32), approximate=True) * up_proj.astype(jnp.float32)).astype(jnp.bfloat16)
    mlp_out = project(activated, w_down)
    hidden = (hidden.astype(jnp.float32) + rms_norm(mlp_out, layer_gains[3]).astype(jnp.float32)).astype(jnp.bfloat16)
    return hidden, new_keys.reshape(batch_size, KV_HEADS * HEAD_DIM), new_values.reshape(batch_size, KV_HEADS * HEAD_DIM)


def reference(tokens, lengths, embed_table, norm_gains, w_query, w_key, w_value, w_out, w_gate, w_up, w_down, key_local, value_local, key_global, value_global):
    normalizer = jnp.asarray(math.sqrt(MODEL_DIM), dtype=jnp.bfloat16).astype(jnp.float32)
    hidden = (jnp.take(embed_table, tokens, axis=0).astype(jnp.float32) * normalizer).astype(jnp.bfloat16)
    hidden, keys_zero, values_zero = decoder_layer(hidden, lengths, norm_gains[0:4], w_query[0], w_key[0], w_value[0], w_out[0], w_gate[0], w_up[0], w_down[0], key_local, value_local, True)
    hidden, keys_one, values_one = decoder_layer(hidden, lengths, norm_gains[4:8], w_query[1], w_key[1], w_value[1], w_out[1], w_gate[1], w_up[1], w_down[1], key_global, value_global, False)
    final_normed = rms_norm(hidden, norm_gains[8])
    raw_logits = jnp.dot(final_normed, embed_table.T, preferred_element_type=jnp.float32)
    logits = 30.0 * jnp.tanh(raw_logits / 30.0)
    return (logits, jnp.stack([keys_zero, keys_one]), jnp.stack([values_zero, values_one]))
```

```python
import functools
import math

import jax
import jax.numpy as jnp
import numpy as np
from jax import lax
from jax.experimental import pallas as pl
from jax.experimental.pallas import tpu as pltpu
from jax.sharding import PartitionSpec as P

MESH = pl.DeviceIdType.MESH
F32, BF16 = jnp.float32, jnp.bfloat16
DIM = 3840
N_DEV = 8
RING = 12
CACHE = 5
PIECE = 768
PIECES = 5
HEAD_ROWS = 512
PER_LAYER = 16
FF_COLS = (512, 512, 512, 384)


def dot(a, b):
    return jnp.dot(a, b, preferred_element_type=F32)


def dot_t(a, b):
    return lax.dot_general(a, b, (((1,), (1,)), ((), ())), preferred_element_type=F32)


def round_bf16(v):
    return v.astype(BF16).astype(F32)


def step_kernel(len_ref, emb_ref, gains_ref, freq_ref, wq, wk, wv, wo, wg, wu, wd, table, kl, vl, kg, vg,
                logits_ref, nk_ref, nv_ref,
                ring, cbuf, recv, ring_sem, c_sem, send_sem, recv_sem):
    me = lax.axis_index("tp")
    head_chunks = table.shape[0] // HEAD_ROWS

    def col_copies(slot, src_a, src_b, off_b, base, width):
        sem = ring_sem.at[slot]
        copies = []
        if src_b is None:
            copies.append((src_a.at[pl.ds(0, 2560), pl.ds(base, width)], ring.at[slot, pl.ds(0, 2560), pl.ds(0, width)]))
            src_b, off_b = src_a, base + 256
        else:
            copies.append((src_a.at[pl.ds(0, 2560), pl.ds(base, 256)], ring.at[slot, pl.ds(0, 2560), pl.ds(0, 256)]))
            copies.append((src_b.at[pl.ds(0, 2560), pl.ds(off_b, 256)], ring.at[slot, pl.ds(0, 2560), pl.ds(256, 256)]))
        copies.append((src_a.at[pl.ds(2560, 1280), pl.ds(base, 256)], ring.at[slot, pl.ds(0, 1280), pl.ds(512, 256)]))
        copies.append((src_b.at[pl.ds(2560, 1280), pl.ds(off_b, width - 256)], ring.at[slot, pl.ds(1280, 1280), pl.ds(512, width - 256)]))
        for src, dst in copies:
            pltpu.make_async_copy(src, dst, sem).start()

    def row_copies(slot, src, row0, rows):
        for j in range(PIECES):
            pltpu.make_async_copy(src.at[pl.ds(row0, rows), pl.ds(PIECE * j, PIECE)],
                                  ring.at[slot, pl.ds(rows * j, rows)], ring_sem.at[slot]).start()

    def issue(i):
        if i >= 2 * PER_LAYER + head_chunks:
            return
        slot = i % RING
        if i >= 2 * PER_LAYER:
            row_copies(slot, table, (i - 2 * PER_LAYER) * HEAD_ROWS, HEAD_ROWS)
            return
        layer, c = divmod(i, PER_LAYER)
        if c == 0:
            col_copies(slot, wq.at[layer], None, 0, 0, 512)
        elif c == 1:
            col_copies(slot, wk.at[layer], wv.at[layer], 0, 0, 512)
        elif c == 2:
            row_copies(slot, wo.at[layer], 0, 512)
        elif c < 11:
            block, which = divmod(c - 3, 2)
            col_copies(slot, (wg, wu)[which].at[layer], None, 0, 512 * block, FF_COLS[block])
        else:
            pltpu.make_async_copy(wd.at[layer, :, pl.ds(PIECE * (c - 11), PIECE)],
                                  ring.at[slot, pl.ds(0, 1920)], ring_sem.at[slot]).start()

    def arrive(i, rows=2560):
        slot = i % RING
        part = ring.at[slot] if rows == 2560 else ring.at[slot, pl.ds(0, rows)]
        pltpu.make_async_copy(part, part, ring_sem.at[slot]).wait()
        return slot

    cache_list = [kl, vl] + [kg.at[b] for b in range(4)] + [vg.at[b] for b in range(4)]

    def issue_cache(i):
        if i < len(cache_list):
            pltpu.make_async_copy(cache_list[i], cbuf.at[i % CACHE], c_sem.at[i % CACHE]).start()

    def arrive_cache(i):
        pltpu.make_async_copy(cache_list[i], cbuf.at[i % CACHE], c_sem.at[i % CACHE]).wait()
        return i % CACHE

    issue(0)
    issue(1)
    issue_cache(0)
    issue_cache(1)
    for i in range(2, RING):
        issue(i)
    for i in range(2, CACHE):
        issue_cache(i)

    barrier = pltpu.get_barrier_semaphore()
    for k in range(1, N_DEV):
        pl.semaphore_signal(barrier, inc=1, device_id={"tp": lax.rem(me + k, N_DEV)}, device_id_type=MESH)
    pl.semaphore_wait(barrier, N_DEV - 1)

    def send(step, piece=None):
        block = recv.at[step, me] if piece is None else recv.at[step, me, piece]
        for k in (7, 6, 5, 4, 3, 2, 1):
            pltpu.make_async_remote_copy(src_ref=block, dst_ref=block, send_sem=send_sem.at[step], recv_sem=recv_sem.at[step],
                                         device_id={"tp": lax.rem(me + k, N_DEV)}, device_id_type=MESH).start()

    row = lax.broadcasted_iota(jnp.int32, (8, 128), 0)
    low_rows = row < 4
    req = jnp.where(low_rows, row, row - 4)

    def tile_to(mask, width):
        return jnp.concatenate([mask] * (width // 128), axis=1) if width > 128 else mask

    low_384 = lax.broadcasted_iota(jnp.int32, (8, 384), 0) < 4
    low_256 = lax.broadcasted_iota(jnp.int32, (8, 256), 0) < 4

    def pack(value):
        return jnp.where(low_384, value[:, :384], value[:, 384:]).astype(BF16)

    def collect(step):
        whole = recv.at[step, pl.ds(0, N_DEV - 1)]
        pltpu.make_async_copy(whole, whole, recv_sem.at[step]).wait()
        parts = []
        for piece in range(PIECES):
            total = recv[step, 0, piece].astype(F32)
            for dev in range(1, N_DEV):
                total = total + recv[step, dev, piece].astype(F32)
            total = round_bf16(total)
            other = pltpu.roll(total, 4, 0)
            parts += [jnp.where(low_384, total, other), jnp.where(low_384, other, total)]
        return jnp.concatenate(parts, axis=1)

    recv[0, me] = emb_ref[...]
    send(0)

    len_row = jnp.full((8, 128), len_ref[3], jnp.int32)
    for b in range(3):
        len_row = jnp.where(req == b, len_ref[b], len_row)
    angle = len_row.astype(F32) * freq_ref[...]
    cos_tab, sin_tab = jnp.cos(angle), jnp.sin(angle)
    len_col = len_row[:, :1]

    def rotate(head):
        lo, hi = head[:, :128], head[:, 128:]
        return jnp.concatenate([lo * cos_tab - hi * sin_tab, hi * cos_tab + lo * sin_tab], axis=1)

    def norm(value, index):
        gain = gains_ref[pl.ds(index, 1), :].astype(F32)
        inv = lax.rsqrt(jnp.mean(value * value, axis=-1, keepdims=True) + 1e-6)
        return (value * inv * (1.0 + gain)).astype(BF16)

    def dot_cols(x, slot, width):
        head, tail = x[:, :2560], x[:, 2560:]
        main = dot(head, ring[slot, :, pl.ds(0, width)])
        left = dot(tail, ring[slot, pl.ds(0, 1280), pl.ds(512, 256)])
        right = dot(tail, ring[slot, pl.ds(1280, 1280), pl.ds(512, width - 256)])
        return main + jnp.concatenate([left, right], axis=1)

    def cap(scores):
        return 50.0 * jnp.tanh(scores / 50.0)

    def finish_attention(q8, scores, new_k, slots, is_local):
        slot_id = lax.broadcasted_iota(jnp.int32, (8, slots), 1)
        valid = slot_id <= len_col
        write = len_col
        if is_local:
            valid = valid | (len_col >= slots - 1)
            write = lax.rem(len_col, slots)
        valid = valid & (slot_id != write)
        capped = jnp.where(valid, cap(scores), -1e30)
        own = cap(jnp.sum(q8.astype(F32) * new_k.astype(F32), axis=-1, keepdims=True))
        top = jnp.maximum(jnp.max(capped, axis=-1, keepdims=True), own)
        grown, own = jnp.exp(capped - top), jnp.exp(own - top)
        total = jnp.sum(grown, axis=-1, keepdims=True) + own
        return (grown / total).astype(BF16), round_bf16(own / total)

    def layer_step(layer, x, is_local):
        base = PER_LAYER * layer
        a = norm(x, 4 * layer)
        slot = arrive(base)
        q = round_bf16(dot_cols(a, slot, 512))
        issue(base + RING)
        slot = arrive(base + 1)
        kv = dot_cols(a, slot, 512).astype(BF16)
        issue(base + 1 + RING)
        new_k = rotate(kv[:, :256].astype(F32)).astype(BF16)
        new_v = kv[:, 256:]
        nk_ref[layer] = new_k[:4]
        nv_ref[layer] = new_v[:4]
        q_both = jnp.where(low_256, q[:, :256], q[:, 256:])
        q8 = (rotate(q_both) * 0.0625).astype(BF16)

        if is_local:
            slots = 1024
            every = dot_t(q8, cbuf[arrive_cache(0)])
            issue_cache(CACHE)
            req_wide = tile_to(req, slots)
            scores = every[:, 3 * slots:]
            for b in range(3):
                scores = jnp.where(req_wide == b, every[:, b * slots:(b + 1) * slots], scores)
        else:
            slots = 4096
            req_wide = tile_to(req, slots)
            scores = None
            for b in range(4):
                one = dot_t(q8, cbuf[arrive_cache(2 + b)])
                issue_cache(2 + b + CACHE)
                scores = one if scores is None else jnp.where(req_wide == b, one, scores)
        probs, own = finish_attention(q8, scores, new_k, slots, is_local)
        mixed = None
        for b in range(4):
            if is_local:
                if b == 0:
                    at = arrive_cache(1)
                one = dot(probs, cbuf[at, pl.ds(b * slots, slots)])
            else:
                one = dot(probs, cbuf[arrive_cache(6 + b)])
            mixed = one if mixed is None else jnp.where(tile_to(req, 256) == b, one, mixed)
            if is_local and b == 3:
                issue_cache(1 + CACHE)
            elif not is_local:
                issue_cache(6 + b + CACHE)
        mixed = round_bf16(mixed + own * new_v.astype(F32))
        other = pltpu.roll(mixed, 4, 0)
        mixed = jnp.concatenate([jnp.where(low_256, mixed, other), jnp.where(low_256, other, mixed)], axis=1).astype(BF16)

        step = 1 + 2 * layer
        slot = arrive(base + 2)
        for j in range(PIECES):
            recv[step, me, j] = pack(dot(mixed, ring[slot, pl.ds(512 * j, 512)]))
        send(step)
        issue(base + 2 + RING)
        x = round_bf16(x + norm(collect(step), 4 * layer + 1).astype(F32))

        a = norm(x, 4 * layer + 2)
        acts = []
        for block, width in enumerate(FF_COLS):
            rows = 2560 if width == 512 else 1920
            at = base + 3 + 2 * block
            gate = round_bf16(dot_cols(a, arrive(at, rows), width))
            issue(at + RING)
            up = round_bf16(dot_cols(a, arrive(at + 1, rows), width))
            issue(at + 1 + RING)
            acts.append((jax.nn.gelu(gate, approximate=True) * up).astype(BF16))
        act = jnp.concatenate(acts, axis=1)
        step = 2 + 2 * layer
        for j in range(PIECES):
            at = base + 11 + j
            slot = arrive(at, 1920)
            recv[step, me, j] = pack(dot(act, ring[slot, pl.ds(0, 1920)]))
            send(step, j)
            issue(at + RING)
        return round_bf16(x + norm(collect(step), 4 * layer + 3).astype(F32))

    x = collect(0)
    x = layer_step(0, x, True)
    x = layer_step(1, x, False)
    z = norm(x, 8)

    def head_step(e, carry):
        slot = lax.rem(2 * PER_LAYER + e, RING)
        pltpu.make_async_copy(ring.at[slot], ring.at[slot], ring_sem.at[slot]).wait()
        acc = dot_t(z[:, :PIECE], ring[slot, pl.ds(0, HEAD_ROWS)])
        for j in range(1, PIECES):
            acc = acc + dot_t(z[:, PIECE * j:PIECE * (j + 1)], ring[slot, pl.ds(HEAD_ROWS * j, HEAD_ROWS)])
        logits_ref[:, pl.ds(pl.multiple_of(e * HEAD_ROWS, HEAD_ROWS), HEAD_ROWS)] = 30.0 * jnp.tanh(acc[:4] / 30.0)
        return carry

    lax.fori_loop(0, head_chunks, head_step, 0)

    for step in range(5):
        whole = recv.at[step, pl.ds(0, N_DEV - 1)]
        pltpu.make_async_copy(whole, whole, send_sem.at[step]).wait()


def device_step(tokens, lengths, table, gains, wq, wk, wv, wo, wg, wu, wd, kl, vl, kg, vg):
    vocab_local = table.shape[0]
    local_ids = tokens - lax.axis_index("tp") * vocab_local
    inside = (local_ids >= 0) & (local_ids < vocab_local)
    picked = jnp.take(table, jnp.clip(local_ids, 0, vocab_local - 1), axis=0)
    normalizer = jnp.asarray(math.sqrt(DIM), dtype=BF16).astype(F32)
    scaled = jnp.where(inside[:, None], picked.astype(F32) * normalizer, 0.0).astype(BF16)
    emb = scaled.reshape(4, PIECES, 2, 384).transpose(1, 2, 0, 3).reshape(PIECES, 8, 384)
    freq = jnp.asarray((10000.0 ** (-2.0 * np.arange(128, dtype=np.float64) / 256)).astype(np.float32)[None])

    def flat(cache):
        return cache.transpose(0, 2, 1, 3).reshape(4, cache.shape[1], 256)

    vmem, hbm = pl.BlockSpec(memory_space=pltpu.VMEM), pl.BlockSpec(memory_space=pl.ANY)
    smem = pl.BlockSpec(memory_space=pltpu.SMEM)
    logits, nk, nv = pl.pallas_call(
        step_kernel,
        out_shape=(jax.ShapeDtypeStruct((4, vocab_local), F32), jax.ShapeDtypeStruct((2, 4, 256), BF16), jax.ShapeDtypeStruct((2, 4, 256), BF16)),
        in_specs=[smem, vmem, vmem, vmem] + [hbm] * 12,
        out_specs=(vmem, vmem, vmem),
        scratch_shapes=[
            pltpu.VMEM((RING, 2560, PIECE), BF16),
            pltpu.VMEM((CACHE, 4096, 256), BF16),
            pltpu.VMEM((5, N_DEV, PIECES, 8, 384), BF16),
            pltpu.SemaphoreType.DMA((RING,)),
            pltpu.SemaphoreType.DMA((CACHE,)),
            pltpu.SemaphoreType.DMA((5,)),
            pltpu.SemaphoreType.DMA((5,)),
        ],
        compiler_params=pltpu.CompilerParams(collective_id=0, has_side_effects=True, vmem_limit_bytes=67_000_000),
    )(lengths, emb, gains, freq, wq, wk, wv, wo, wg, wu, wd, table,
      flat(kl).reshape(-1, 256), flat(vl).reshape(-1, 256), flat(kg), flat(vg))
    return logits, nk, nv


def solution(mesh):
    cache_spec = P("dp", None, "tp", None)
    col_spec = P(None, None, "tp")
    row_spec = P(None, "tp", None)
    rows_spec = P(None, "dp", "tp")
    in_specs = (P("dp"), P("dp"), P("tp", None), P(), col_spec, col_spec, col_spec, row_spec, col_spec, col_spec, row_spec,
                cache_spec, cache_spec, cache_spec, cache_spec)
    out_specs = (P("dp", "tp"), rows_spec, rows_spec)
    return jax.shard_map(device_step, mesh=mesh, in_specs=in_specs, out_specs=out_specs, check_vma=False)
```

```python
import functools
import math

import jax
import jax.numpy as jnp
import numpy as np
from jax import lax
from jax.experimental import pallas as pl
from jax.experimental.pallas import tpu as pltpu
from jax.sharding import PartitionSpec as P

MESH = pl.DeviceIdType.MESH
F32, BF16 = jnp.float32, jnp.bfloat16
DIM = 3840
N_DEV = 8
RING = 10
CACHE = 10
PIECE = 768
PIECES = 5
HEAD_ROWS = 512
PER_LAYER = 16
FF_COLS = (512, 512, 512, 384)


def dot(a, b):
    return jnp.dot(a, b, preferred_element_type=F32)


def dot_t(a, b):
    return lax.dot_general(a, b, (((1,), (1,)), ((), ())), preferred_element_type=F32)


def round_bf16(v):
    return v.astype(BF16).astype(F32)


def step_kernel(len_ref, emb_ref, gains_ref, freq_ref, wq, wk, wv, wo, wg, wu, wd, table, kl, vl, kg, vg,
                logits_ref, nk_ref, nv_ref,
                ring, cbuf, recv, gain_buf, freq_buf, ring_sem, c_sem, send_sem, recv_sem, small_sem):
    me = lax.axis_index("tp")
    head_chunks = table.shape[0] // HEAD_ROWS

    def col_copies(slot, src_a, src_b, off_b, base, width):
        sem = ring_sem.at[slot]
        copies = []
        if src_b is None:
            copies.append((src_a.at[pl.ds(0, 2560), pl.ds(base, width)], ring.at[slot, pl.ds(0, 2560), pl.ds(0, width)]))
            src_b, off_b = src_a, base + 256
        else:
            copies.append((src_a.at[pl.ds(0, 2560), pl.ds(base, 256)], ring.at[slot, pl.ds(0, 2560), pl.ds(0, 256)]))
            copies.append((src_b.at[pl.ds(0, 2560), pl.ds(off_b, 256)], ring.at[slot, pl.ds(0, 2560), pl.ds(256, 256)]))
        copies.append((src_a.at[pl.ds(2560, 1280), pl.ds(base, 256)], ring.at[slot, pl.ds(0, 1280), pl.ds(512, 256)]))
        copies.append((src_b.at[pl.ds(2560, 1280), pl.ds(off_b, width - 256)], ring.at[slot, pl.ds(1280, 1280), pl.ds(512, width - 256)]))
        for src, dst in copies:
            pltpu.make_async_copy(src, dst, sem).start()

    def row_copies(slot, src, row0, rows):
        for j in range(PIECES):
            pltpu.make_async_copy(src.at[pl.ds(row0, rows), pl.ds(PIECE * j, PIECE)],
                                  ring.at[slot, pl.ds(rows * j, rows)], ring_sem.at[slot]).start()

    def issue(i):
        if i >= 2 * PER_LAYER + head_chunks:
            return
        slot = i % RING
        if i >= 2 * PER_LAYER:
            row_copies(slot, table, (i - 2 * PER_LAYER) * HEAD_ROWS, HEAD_ROWS)
            return
        layer, c = divmod(i, PER_LAYER)
        if c == 0:
            col_copies(slot, wq.at[layer], None, 0, 0, 512)
        elif c == 1:
            col_copies(slot, wk.at[layer], wv.at[layer], 0, 0, 512)
        elif c == 2:
            row_copies(slot, wo.at[layer], 0, 512)
        elif c < 11:
            block, which = divmod(c - 3, 2)
            col_copies(slot, (wg, wu)[which].at[layer], None, 0, 512 * block, FF_COLS[block])
        else:
            pltpu.make_async_copy(wd.at[layer, :, pl.ds(PIECE * (c - 11), PIECE)],
                                  ring.at[slot, pl.ds(0, 1920)], ring_sem.at[slot]).start()

    def arrive(i, rows=2560):
        slot = i % RING
        part = ring.at[slot] if rows == 2560 else ring.at[slot, pl.ds(0, rows)]
        pltpu.make_async_copy(part, part, ring_sem.at[slot]).wait()
        return slot

    cache_list = [kl, vl] + [kg.at[b] for b in range(4)] + [vg.at[b] for b in range(4)]

    def issue_cache(i):
        pltpu.make_async_copy(cache_list[i], cbuf.at[i], c_sem.at[i]).start()

    def arrive_cache(i):
        pltpu.make_async_copy(cache_list[i], cbuf.at[i], c_sem.at[i]).wait()
        return i

    core, x_pos, y_pos = lax.rem(me, 2), lax.rem(me // 2, 2), me // 4
    far = [(1 - y_pos, 1 - x_pos, core), (1 - y_pos, 1 - x_pos, 1 - core)]
    near = [(y_pos, 1 - x_pos, core), (1 - y_pos, x_pos, core), (y_pos, 1 - x_pos, 1 - core), (1 - y_pos, x_pos, 1 - core)]
    peers = [(py * 2 + px) * 2 + pc for py, px, pc in far + near + [(y_pos, x_pos, 1 - core)]]

    barrier = pltpu.get_barrier_semaphore()
    for peer in peers:
        pl.semaphore_signal(barrier, inc=1, device_id={"tp": peer}, device_id_type=MESH)

    issue(0)
    gain_copy = pltpu.make_async_copy(gains_ref, gain_buf, small_sem.at[1])
    gain_copy.start()
    freq_copy = pltpu.make_async_copy(freq_ref, freq_buf, small_sem.at[0])
    freq_copy.start()
    issue(1)

    @pl.when(me >= 0)
    def _():
        issue_cache(0)
        issue_cache(1)
        issue(2)

    for i in range(3, RING):
        pl.when(me >= 0)(functools.partial(issue, i))

    @pl.when(me >= 0)
    def _():
        for i in range(2, CACHE):
            issue_cache(i)

    recv[0, me] = emb_ref[...]
    pl.semaphore_wait(barrier, N_DEV - 1)

    def send(step, piece=None):
        block = recv.at[step, me] if piece is None else recv.at[step, me, piece]
        for peer in peers:
            pltpu.make_async_remote_copy(src_ref=block, dst_ref=block, send_sem=send_sem.at[step], recv_sem=recv_sem.at[step],
                                         device_id={"tp": peer}, device_id_type=MESH).start()

    row = lax.broadcasted_iota(jnp.int32, (8, 128), 0)
    low_rows = row < 4
    req = jnp.where(low_rows, row, row - 4)

    def tile_to(mask, width):
        return jnp.concatenate([mask] * (width // 128), axis=1) if width > 128 else mask

    low_384 = lax.broadcasted_iota(jnp.int32, (8, 384), 0) < 4
    low_256 = lax.broadcasted_iota(jnp.int32, (8, 256), 0) < 4

    def pack(value):
        return jnp.where(low_384, value[:, :384], value[:, 384:]).astype(BF16)

    def collect(step):
        whole = recv.at[step, pl.ds(0, N_DEV - 1)]
        pltpu.make_async_copy(whole, whole, recv_sem.at[step]).wait()
        parts = []
        for piece in range(PIECES):
            total = recv[step, 0, piece].astype(F32)
            for dev in range(1, N_DEV):
                total = total + recv[step, dev, piece].astype(F32)
            total = round_bf16(total)
            other = pltpu.roll(total, 4, 0)
            parts += [jnp.where(low_384, total, other), jnp.where(low_384, other, total)]
        return jnp.concatenate(parts, axis=1)

    send(0)
    gain_copy.wait()
    freq_copy.wait()

    len_row = jnp.full((8, 128), len_ref[3], jnp.int32)
    for b in range(3):
        len_row = jnp.where(req == b, len_ref[b], len_row)
    angle = len_row.astype(F32) * freq_buf[...]
    cos_tab, sin_tab = jnp.cos(angle), jnp.sin(angle)
    len_col = len_row[:, :1]

    def rotate(head):
        lo, hi = head[:, :128], head[:, 128:]
        return jnp.concatenate([lo * cos_tab - hi * sin_tab, hi * cos_tab + lo * sin_tab], axis=1)

    def norm(value, index):
        gain = gain_buf[pl.ds(index, 1), :].astype(F32)
        inv = lax.rsqrt(jnp.mean(value * value, axis=-1, keepdims=True) + 1e-6)
        return (value * inv * (1.0 + gain)).astype(BF16)

    def dot_cols(x, slot, width):
        head, tail = x[:, :2560], x[:, 2560:]
        main = dot(head, ring[slot, :, pl.ds(0, width)])
        left = dot(tail, ring[slot, pl.ds(0, 1280), pl.ds(512, 256)])
        right = dot(tail, ring[slot, pl.ds(1280, 1280), pl.ds(512, width - 256)])
        return main + jnp.concatenate([left, right], axis=1)

    def cap(scores):
        return 50.0 * jnp.tanh(scores / 50.0)

    def finish_attention(q8, scores, new_k, slots, is_local):
        slot_id = lax.broadcasted_iota(jnp.int32, (8, slots), 1)
        valid = slot_id <= len_col
        write = len_col
        if is_local:
            valid = valid | (len_col >= slots - 1)
            write = lax.rem(len_col, slots)
        valid = valid & (slot_id != write)
        capped = jnp.where(valid, cap(scores), -1e30)
        own = cap(jnp.sum(q8.astype(F32) * new_k.astype(F32), axis=-1, keepdims=True))
        top = jnp.maximum(jnp.max(capped, axis=-1, keepdims=True), own)
        grown, own = jnp.exp(capped - top), jnp.exp(own - top)
        total = jnp.sum(grown, axis=-1, keepdims=True) + own
        return (grown / total).astype(BF16), round_bf16(own / total)

    def layer_step(layer, x, is_local):
        base = PER_LAYER * layer
        a = norm(x, 4 * layer)
        slot = arrive(base)
        q = round_bf16(dot_cols(a, slot, 512))
        issue(base + RING)
        slot = arrive(base + 1)
        kv = dot_cols(a, slot, 512).astype(BF16)
        issue(base + 1 + RING)
        new_k = rotate(kv[:, :256].astype(F32)).astype(BF16)
        new_v = kv[:, 256:]
        nk_ref[layer] = new_k[:4]
        nv_ref[layer] = new_v[:4]
        q_both = jnp.where(low_256, q[:, :256], q[:, 256:])
        q8 = (rotate(q_both) * 0.0625).astype(BF16)

        if is_local:
            slots = 1024
            every = dot_t(q8, cbuf[arrive_cache(0)])
            req_wide = tile_to(req, slots)
            scores = every[:, 3 * slots:]
            for b in range(3):
                scores = jnp.where(req_wide == b, every[:, b * slots:(b + 1) * slots], scores)
        else:
            slots = 4096
            req_wide = tile_to(req, slots)
            scores = None
            for b in range(4):
                one = dot_t(q8, cbuf[arrive_cache(2 + b)])
                scores = one if scores is None else jnp.where(req_wide == b, one, scores)
        probs, own = finish_attention(q8, scores, new_k, slots, is_local)
        mixed = None
        for b in range(4):
            if is_local:
                if b == 0:
                    at = arrive_cache(1)
                one = dot(probs, cbuf[at, pl.ds(b * slots, slots)])
            else:
                one = dot(probs, cbuf[arrive_cache(6 + b)])
            mixed = one if mixed is None else jnp.where(tile_to(req, 256) == b, one, mixed)
        mixed = round_bf16(mixed + own * new_v.astype(F32))
        other = pltpu.roll(mixed, 4, 0)
        mixed = jnp.concatenate([jnp.where(low_256, mixed, other), jnp.where(low_256, other, mixed)], axis=1).astype(BF16)

        step = 1 + 2 * layer
        slot = arrive(base + 2)
        for j in range(PIECES):
            recv[step, me, j] = pack(dot(mixed, ring[slot, pl.ds(512 * j, 512)]))
        send(step)
        issue(base + 2 + RING)
        x = round_bf16(x + norm(collect(step), 4 * layer + 1).astype(F32))

        a = norm(x, 4 * layer + 2)
        acts = []
        for block, width in enumerate(FF_COLS):
            rows = 2560 if width == 512 else 1920
            at = base + 3 + 2 * block
            gate = round_bf16(dot_cols(a, arrive(at, rows), width))
            issue(at + RING)
            up = round_bf16(dot_cols(a, arrive(at + 1, rows), width))
            issue(at + 1 + RING)
            acts.append((jax.nn.gelu(gate, approximate=True) * up).astype(BF16))
        act = jnp.concatenate(acts, axis=1)
        step = 2 + 2 * layer
        for j in range(PIECES):
            at = base + 11 + j
            slot = arrive(at, 1920)
            recv[step, me, j] = pack(dot(act, ring[slot, pl.ds(0, 1920)]))
            send(step, j)
            issue(at + RING)
        return round_bf16(x + norm(collect(step), 4 * layer + 3).astype(F32))

    x = collect(0)
    x = layer_step(0, x, True)
    x = layer_step(1, x, False)
    z = norm(x, 8)

    def head_step(e, carry):
        slot = lax.rem(2 * PER_LAYER + e, RING)
        pltpu.make_async_copy(ring.at[slot], ring.at[slot], ring_sem.at[slot]).wait()
        acc = dot_t(z[:, :PIECE], ring[slot, pl.ds(0, HEAD_ROWS)])
        for j in range(1, PIECES):
            acc = acc + dot_t(z[:, PIECE * j:PIECE * (j + 1)], ring[slot, pl.ds(HEAD_ROWS * j, HEAD_ROWS)])
        logits_ref[:, pl.ds(pl.multiple_of(e * HEAD_ROWS, HEAD_ROWS), HEAD_ROWS)] = 30.0 * jnp.tanh(acc[:4] / 30.0)

        @pl.when(e < head_chunks - RING)
        def _():
            row_copies(slot, table, pl.multiple_of((e + RING) * HEAD_ROWS, HEAD_ROWS), HEAD_ROWS)

        return carry

    lax.fori_loop(0, head_chunks, head_step, 0)

    for step in range(5):
        whole = recv.at[step, pl.ds(0, N_DEV - 1)]
        pltpu.make_async_copy(whole, whole, send_sem.at[step]).wait()


def embed_kernel(token_ref, table, out_ref, block, sem):
    rows = table.shape[0]
    first = lax.axis_index("tp") * rows
    ids, copies = [], []
    for b in range(4):
        local = token_ref[b] - first
        safe = jnp.clip(local, 0, rows - 1)
        base = pl.multiple_of((safe // 8) * 8, 8)
        copy = pltpu.make_async_copy(table.at[pl.ds(base, 8)], block.at[b], sem.at[b])
        copy.start()
        copies.append(copy)
        ids.append(jnp.where((local >= 0) & (local < rows), safe - base, -1))
    row = lax.broadcasted_iota(jnp.int32, (8, DIM), 0)
    scale = float(np.asarray(math.sqrt(DIM), np.float32).astype(BF16))
    full = jnp.zeros((8, DIM), F32)
    for b in range(4):
        copies[b].wait()
        mine = jnp.sum(jnp.where(row == ids[b], block[b].astype(F32), 0.0), axis=0, keepdims=True)
        full = jnp.where((row == b) | (row == b + 4), mine * scale, full)
    low = lax.broadcasted_iota(jnp.int32, (8, 384), 0) < 4
    for j in range(PIECES):
        out_ref[j] = jnp.where(low, full[:, PIECE * j:PIECE * j + 384], full[:, PIECE * j + 384:PIECE * (j + 1)]).astype(BF16)


def pass_kernel(a_in, b_in, c_in, a_out, b_out, c_out, sem):
    copies = [pltpu.make_async_copy(src, dst, sem.at[i]) for i, (src, dst) in enumerate(((a_in, a_out), (b_in, b_out), (c_in, c_out)))]
    for copy in copies:
        copy.start()
    for copy in copies:
        copy.wait()


def device_step(tokens, lengths, table, gains, wq, wk, wv, wo, wg, wu, wd, kl, vl, kg, vg):
    vocab_local = table.shape[0]
    vmem, hbm = pl.BlockSpec(memory_space=pltpu.VMEM), pl.BlockSpec(memory_space=pl.ANY)
    smem = pl.BlockSpec(memory_space=pltpu.SMEM)
    emb = pl.pallas_call(
        embed_kernel,
        out_shape=pltpu.VMEM((PIECES, 8, 384), BF16),
        in_specs=[smem, hbm],
        out_specs=vmem,
        scratch_shapes=[pltpu.VMEM((4, 8, DIM), BF16), pltpu.SemaphoreType.DMA((4,))],
    )(tokens, table)
    freq = jnp.asarray((10000.0 ** (-2.0 * np.arange(128, dtype=np.float64) / 256)).astype(np.float32)[None])

    def flat(cache):
        return cache.transpose(0, 2, 1, 3).reshape(4, cache.shape[1], 256)

    results = (jax.ShapeDtypeStruct((4, vocab_local), F32), jax.ShapeDtypeStruct((2, 4, 256), BF16), jax.ShapeDtypeStruct((2, 4, 256), BF16))
    logits, nk, nv = pl.pallas_call(
        step_kernel,
        out_shape=tuple(pltpu.VMEM(r.shape, r.dtype) for r in results),
        in_specs=[smem, vmem] + [hbm] * 14,
        out_specs=(vmem, vmem, vmem),
        scratch_shapes=[
            pltpu.VMEM((RING, 2560, PIECE), BF16),
            pltpu.VMEM((CACHE, 4096, 256), BF16),
            pltpu.VMEM((5, N_DEV, PIECES, 8, 384), BF16),
            pltpu.VMEM((9, DIM), BF16),
            pltpu.VMEM((1, 128), F32),
            pltpu.SemaphoreType.DMA((RING,)),
            pltpu.SemaphoreType.DMA((CACHE,)),
            pltpu.SemaphoreType.DMA((5,)),
            pltpu.SemaphoreType.DMA((5,)),
            pltpu.SemaphoreType.DMA((2,)),
        ],
        compiler_params=pltpu.CompilerParams(collective_id=0, has_side_effects=True, vmem_limit_bytes=64_500_000),
    )(lengths, pltpu.with_memory_space_constraint(emb, pltpu.VMEM), gains, freq, wq, wk, wv, wo, wg, wu, wd, table,
      flat(kl).reshape(-1, 256), flat(vl).reshape(-1, 256), flat(kg), flat(vg))
    keep = [pltpu.with_memory_space_constraint(v, pltpu.VMEM) for v in (logits, nk, nv)]
    return pl.pallas_call(
        pass_kernel,
        out_shape=results,
        in_specs=[vmem] * 3,
        out_specs=(hbm,) * 3,
        scratch_shapes=[pltpu.SemaphoreType.DMA((3,))],
    )(*keep)


def solution(mesh):
    cache_spec = P("dp", None, "tp", None)
    col_spec = P(None, None, "tp")
    row_spec = P(None, "tp", None)
    rows_spec = P(None, "dp", "tp")
    in_specs = (P("dp"), P("dp"), P("tp", None), P(), col_spec, col_spec, col_spec, row_spec, col_spec, col_spec, row_spec,
                cache_spec, cache_spec, cache_spec, cache_spec)
    out_specs = (P("dp", "tp"), rows_spec, rows_spec)
    return jax.shard_map(device_step, mesh=mesh, in_specs=in_specs, out_specs=out_specs, check_vma=False)
```

```python
import functools
import math

import jax
import jax.numpy as jnp
import numpy as np
from jax import lax
from jax.experimental import pallas as pl
from jax.experimental.pallas import tpu as pltpu
from jax.sharding import PartitionSpec as P

MESH = pl.DeviceIdType.MESH
F32, BF16 = jnp.float32, jnp.bfloat16
DIM = 3840
N_DEV = 8
RING = 10
CACHE = 10
PIECE = 768
PIECES = 5
HEAD_ROWS = 512
HEAD_EARLY = 6
PER_LAYER = 16
FF_COLS = (512, 512, 512, 384)


def dot(a, b):
    return jnp.dot(a, b, preferred_element_type=F32)


def dot_t(a, b):
    return lax.dot_general(a, b, (((1,), (1,)), ((), ())), preferred_element_type=F32)


def round_bf16(v):
    return v.astype(BF16).astype(F32)


def step_kernel(len_ref, emb_ref, gains_ref, freq_ref, wq, wk, wv, wo, wg, wu, wd, table, kl, vl, kg, vg,
                z_out, nk_ref, nv_ref, ring,
                cbuf, recv, gain_buf, freq_buf, ring_sem, c_sem, send_sem, recv_sem, small_sem):
    me = lax.axis_index("tp")

    def col_copies(slot, src_a, src_b, off_b, base, width):
        sem = ring_sem.at[slot]
        copies = []
        if src_b is None:
            copies.append((src_a.at[pl.ds(0, 2560), pl.ds(base, width)], ring.at[slot, pl.ds(0, 2560), pl.ds(0, width)]))
            src_b, off_b = src_a, base + 256
        else:
            copies.append((src_a.at[pl.ds(0, 2560), pl.ds(base, 256)], ring.at[slot, pl.ds(0, 2560), pl.ds(0, 256)]))
            copies.append((src_b.at[pl.ds(0, 2560), pl.ds(off_b, 256)], ring.at[slot, pl.ds(0, 2560), pl.ds(256, 256)]))
        copies.append((src_a.at[pl.ds(2560, 1280), pl.ds(base, 256)], ring.at[slot, pl.ds(0, 1280), pl.ds(512, 256)]))
        copies.append((src_b.at[pl.ds(2560, 1280), pl.ds(off_b, width - 256)], ring.at[slot, pl.ds(1280, 1280), pl.ds(512, width - 256)]))
        for src, dst in copies:
            pltpu.make_async_copy(src, dst, sem).start()

    def row_copies(slot, src, row0, rows):
        for j in range(PIECES):
            pltpu.make_async_copy(src.at[pl.ds(row0, rows), pl.ds(PIECE * j, PIECE)],
                                  ring.at[slot, pl.ds(rows * j, rows)], ring_sem.at[slot]).start()

    def issue(i):
        if i >= 2 * PER_LAYER + HEAD_EARLY:
            return
        slot = i % RING
        if i >= 2 * PER_LAYER:
            row_copies(slot, table, (i - 2 * PER_LAYER) * HEAD_ROWS, HEAD_ROWS)
            return
        layer, c = divmod(i, PER_LAYER)
        if c == 0:
            col_copies(slot, wq.at[layer], None, 0, 0, 512)
        elif c == 1:
            col_copies(slot, wk.at[layer], wv.at[layer], 0, 0, 512)
        elif c == 2:
            row_copies(slot, wo.at[layer], 0, 512)
        elif c < 11:
            block, which = divmod(c - 3, 2)
            col_copies(slot, (wg, wu)[which].at[layer], None, 0, 512 * block, FF_COLS[block])
        else:
            pltpu.make_async_copy(wd.at[layer, :, pl.ds(PIECE * (c - 11), PIECE)],
                                  ring.at[slot, pl.ds(0, 1920)], ring_sem.at[slot]).start()

    def arrive(i, rows=2560):
        slot = i % RING
        part = ring.at[slot] if rows == 2560 else ring.at[slot, pl.ds(0, rows)]
        pltpu.make_async_copy(part, part, ring_sem.at[slot]).wait()
        return slot

    cache_list = [kl, vl] + [kg.at[b] for b in range(4)] + [vg.at[b] for b in range(4)]

    def issue_cache(i):
        pltpu.make_async_copy(cache_list[i], cbuf.at[i], c_sem.at[i]).start()

    def arrive_cache(i):
        pltpu.make_async_copy(cache_list[i], cbuf.at[i], c_sem.at[i]).wait()
        return i

    core, x_pos, y_pos = lax.rem(me, 2), lax.rem(me // 2, 2), me // 4
    far = [(1 - y_pos, 1 - x_pos, core), (1 - y_pos, 1 - x_pos, 1 - core)]
    near = [(y_pos, 1 - x_pos, core), (1 - y_pos, x_pos, core), (y_pos, 1 - x_pos, 1 - core), (1 - y_pos, x_pos, 1 - core)]
    peers = [(py * 2 + px) * 2 + pc for py, px, pc in far + near + [(y_pos, x_pos, 1 - core)]]

    barrier = pltpu.get_barrier_semaphore()
    for peer in peers:
        pl.semaphore_signal(barrier, inc=1, device_id={"tp": peer}, device_id_type=MESH)

    def start(chunks, caches=()):
        @pl.when(me >= 0)
        def _():
            for i in chunks:
                issue(i)
            for i in caches:
                issue_cache(i)

    gain_copy = pltpu.make_async_copy(gains_ref, gain_buf, small_sem.at[1])
    freq_copy = pltpu.make_async_copy(freq_ref, freq_buf, small_sem.at[0])
    start((0,))
    gain_copy.start()
    freq_copy.start()
    start((1,), (0, 1))
    recv[0, me] = emb_ref[...]
    pl.semaphore_wait(barrier, N_DEV - 1)

    def send(step, piece=None):
        block = recv.at[step, me] if piece is None else recv.at[step, me, piece]
        for peer in peers:
            pltpu.make_async_remote_copy(src_ref=block, dst_ref=block, send_sem=send_sem.at[step], recv_sem=recv_sem.at[step],
                                         device_id={"tp": peer}, device_id_type=MESH).start()

    row = lax.broadcasted_iota(jnp.int32, (8, 128), 0)
    low_rows = row < 4
    req = jnp.where(low_rows, row, row - 4)

    def tile_to(mask, width):
        return jnp.concatenate([mask] * (width // 128), axis=1) if width > 128 else mask

    low_384 = lax.broadcasted_iota(jnp.int32, (8, 384), 0) < 4
    low_256 = lax.broadcasted_iota(jnp.int32, (8, 256), 0) < 4

    def pack(value):
        return jnp.where(low_384, value[:, :384], value[:, 384:]).astype(BF16)

    def collect(step):
        whole = recv.at[step, pl.ds(0, N_DEV - 1)]
        pltpu.make_async_copy(whole, whole, recv_sem.at[step]).wait()
        parts = []
        for piece in range(PIECES):
            total = recv[step, 0, piece].astype(F32)
            for dev in range(1, N_DEV):
                total = total + recv[step, dev, piece].astype(F32)
            total = round_bf16(total)
            other = pltpu.roll(total, 4, 0)
            parts += [jnp.where(low_384, total, other), jnp.where(low_384, other, total)]
        return jnp.concatenate(parts, axis=1)

    send(0)
    for i in range(2, RING):
        start((i,))
    gain_copy.wait()
    freq_copy.wait()

    len_row = jnp.full((8, 128), len_ref[3], jnp.int32)
    for b in range(3):
        len_row = jnp.where(req == b, len_ref[b], len_row)
    angle = len_row.astype(F32) * freq_buf[...]
    cos_tab, sin_tab = jnp.cos(angle), jnp.sin(angle)
    len_col = len_row[:, :1]

    def rotate(head):
        lo, hi = head[:, :128], head[:, 128:]
        return jnp.concatenate([lo * cos_tab - hi * sin_tab, hi * cos_tab + lo * sin_tab], axis=1)

    def norm(value, index):
        gain = gain_buf[pl.ds(index, 1), :].astype(F32)
        inv = lax.rsqrt(jnp.mean(value * value, axis=-1, keepdims=True) + 1e-6)
        return (value * inv * (1.0 + gain)).astype(BF16)

    def dot_cols(x, slot, width):
        head, tail = x[:, :2560], x[:, 2560:]
        main = dot(head, ring[slot, :, pl.ds(0, width)])
        left = dot(tail, ring[slot, pl.ds(0, 1280), pl.ds(512, 256)])
        right = dot(tail, ring[slot, pl.ds(1280, 1280), pl.ds(512, width - 256)])
        return main + jnp.concatenate([left, right], axis=1)

    def dot_piece(x, slot, row0, rows):
        half = 256 * ((rows + 256) // 512)
        left = dot(x, ring[slot, pl.ds(row0, rows), pl.ds(0, 512)])
        one = dot(x[:, :half], ring[slot, pl.ds(row0, half), pl.ds(512, 256)])
        two = dot(-x[:, half:], ring[slot, pl.ds(row0 + half, rows - half), pl.ds(512, 256)])
        return jnp.concatenate([left, one - two], axis=1)

    def cap(scores):
        return 50.0 * jnp.tanh(scores / 50.0)

    def finish_attention(q8, scores, new_k, slots, is_local):
        slot_id = lax.broadcasted_iota(jnp.int32, (8, slots), 1)
        valid = slot_id <= len_col
        write = len_col
        if is_local:
            valid = valid | (len_col >= slots - 1)
            write = lax.rem(len_col, slots)
        valid = valid & (slot_id != write)
        capped = jnp.where(valid, cap(scores), -1e30)
        own = cap(jnp.sum(q8.astype(F32) * new_k.astype(F32), axis=-1, keepdims=True))
        top = jnp.maximum(jnp.max(capped, axis=-1, keepdims=True), own)
        grown, own = jnp.exp(capped - top), jnp.exp(own - top)
        total = jnp.sum(grown, axis=-1, keepdims=True) + own
        return (grown / total).astype(BF16), round_bf16(own / total)

    def layer_step(layer, x, is_local):
        base = PER_LAYER * layer
        a = norm(x, 4 * layer)
        slot = arrive(base)
        q = round_bf16(dot_cols(a, slot, 512))
        slot = arrive(base + 1)
        kv = dot_cols(a, slot, 512).astype(BF16)
        start((base + RING, base + 1 + RING))
        new_k = rotate(kv[:, :256].astype(F32)).astype(BF16)
        new_v = kv[:, 256:]
        nk_ref[layer] = new_k[:4]
        nv_ref[layer] = new_v[:4]
        q_both = jnp.where(low_256, q[:, :256], q[:, 256:])
        q8 = (rotate(q_both) * 0.0625).astype(BF16)

        if is_local:
            slots = 1024
            every = dot_t(q8, cbuf[arrive_cache(0)])
            req_wide = tile_to(req, slots)
            scores = every[:, 3 * slots:]
            for b in range(3):
                scores = jnp.where(req_wide == b, every[:, b * slots:(b + 1) * slots], scores)
        else:
            slots = 4096
            req_wide = tile_to(req, slots)
            scores = None
            for b in range(4):
                one = dot_t(q8, cbuf[arrive_cache(2 + b)])
                scores = one if scores is None else jnp.where(req_wide == b, one, scores)
        probs, own = finish_attention(q8, scores, new_k, slots, is_local)
        mixed = None
        for b in range(4):
            if is_local:
                if b == 0:
                    at = arrive_cache(1)
                one = dot(probs, cbuf[at, pl.ds(b * slots, slots)])
            else:
                at = arrive_cache(6 + b)
                one = dot(probs[:, :2048], cbuf[at, pl.ds(0, 2048)]) - dot(-probs[:, 2048:], cbuf[at, pl.ds(2048, 2048)])
            mixed = one if mixed is None else jnp.where(tile_to(req, 256) == b, one, mixed)
        mixed = round_bf16(mixed + own * new_v.astype(F32))
        other = pltpu.roll(mixed, 4, 0)
        mixed = jnp.concatenate([jnp.where(low_256, mixed, other), jnp.where(low_256, other, mixed)], axis=1).astype(BF16)

        step = 1 + 2 * layer
        slot = arrive(base + 2)
        for j in range(PIECES):
            recv[step, me, j] = pack(dot_piece(mixed, slot, 512 * j, 512))
            send(step, j)
        start((base + 2 + RING,))
        x = round_bf16(x + norm(collect(step), 4 * layer + 1).astype(F32))

        a = norm(x, 4 * layer + 2)
        acts = []
        for block, width in enumerate(FF_COLS):
            rows = 2560 if width == 512 else 1920
            at = base + 3 + 2 * block
            gate_slot, up_slot = arrive(at, rows), arrive(at + 1, rows)
            gate = round_bf16(dot_cols(a, gate_slot, width))
            up = round_bf16(dot_cols(a, up_slot, width))
            start((at + RING, at + 1 + RING), (2 + 2 * block, 3 + 2 * block) if is_local else ())
            acts.append((jax.nn.gelu(gate, approximate=True) * up).astype(BF16))
        act = jnp.concatenate(acts, axis=1)
        step = 2 + 2 * layer
        for j in range(PIECES):
            at = base + 11 + j
            slot = arrive(at, 1920)
            recv[step, me, j] = pack(dot_piece(act, slot, 0, 1920))
            send(step, j)
            start((at + RING,))
        return round_bf16(x + norm(collect(step), 4 * layer + 3).astype(F32))

    x = collect(0)
    x = layer_step(0, x, True)
    x = layer_step(1, x, False)
    z = norm(x, 8)
    z_out[...] = jnp.concatenate([z, z], axis=0)
    for i in range(HEAD_EARLY):
        arrive(2 * PER_LAYER + i)

    for step in range(5):
        whole = recv.at[step, pl.ds(0, N_DEV - 1)]
        pltpu.make_async_copy(whole, whole, send_sem.at[step]).wait()


def embed_kernel(token_ref, table, out_ref, block, sem):
    rows = table.shape[0]
    first = lax.axis_index("tp") * rows
    ids, copies = [], []
    for b in range(4):
        local = token_ref[b] - first
        safe = jnp.clip(local, 0, rows - 1)
        base = pl.multiple_of((safe // 8) * 8, 8)
        copy = pltpu.make_async_copy(table.at[pl.ds(base, 8)], block.at[b], sem.at[b])
        copy.start()
        copies.append(copy)
        ids.append(jnp.where((local >= 0) & (local < rows), safe - base, -1))
    row = lax.broadcasted_iota(jnp.int32, (8, DIM), 0)
    scale = float(np.asarray(math.sqrt(DIM), np.float32).astype(BF16))
    full = jnp.zeros((8, DIM), F32)
    for b in range(4):
        copies[b].wait()
        mine = jnp.sum(jnp.where(row == ids[b], block[b].astype(F32), 0.0), axis=0, keepdims=True)
        full = jnp.where((row == b) | (row == b + 4), mine * scale, full)
    low = lax.broadcasted_iota(jnp.int32, (8, 384), 0) < 4
    for j in range(PIECES):
        out_ref[j] = jnp.where(low, full[:, PIECE * j:PIECE * j + 384], full[:, PIECE * j + 384:PIECE * (j + 1)]).astype(BF16)


def head_kernel(z_ref, early, nk_in, nv_in, table, logits_out, nk_out, nv_out, late, turned, logits_ref, late_sem, out_sem):
    chunks = table.shape[0] // HEAD_ROWS
    pairs, depth = chunks // 2, DIM // 256
    for i in range(chunks - HEAD_EARLY):
        for j in range(PIECES):
            pltpu.make_async_copy(table.at[pl.ds((HEAD_EARLY + i) * HEAD_ROWS, HEAD_ROWS), pl.ds(PIECE * j, PIECE)],
                                  late.at[i, pl.ds(HEAD_ROWS * j, HEAD_ROWS)], late_sem.at[i]).start()
    keep = [pltpu.make_async_copy(nk_in, nk_out, out_sem.at[0]), pltpu.make_async_copy(nv_in, nv_out, out_sem.at[1])]
    for copy in keep:
        copy.start()

    turned[:, pl.ds(128, 128)] = jnp.zeros((DIM, 128), BF16)
    for j in range(DIM // 128):
        block = jnp.concatenate([z_ref[:, pl.ds(128 * j, 128)].astype(F32), jnp.zeros((112, 128), F32)], axis=0)
        turned[pl.ds(128 * j, 128), pl.ds(0, 128)] = block.T.astype(BF16)

    def part(chunk, row0, rows, c):
        span = pl.ds(row0, rows), pl.ds(256 * c, 256)
        if chunk < HEAD_EARLY:
            return early[(2 * PER_LAYER + chunk) % RING, span[0], span[1]]
        return late[chunk - HEAD_EARLY, span[0], span[1]]

    def unit(q, acc_a, acc_b, need):
        order = [(p, k) for p in range(pairs) for k in range((q + p) % 2, depth, 2)]

        def push(value, register, transpose=False):
            pltpu.matmul_push_rhs(value, staging_register=register, mxu_index=q, transpose=transpose)

        def weights(p, k, half):
            return part(2 * p, HEAD_ROWS * (k // 3) + 256 * half, 256, k % 3)

        def turned_block(k):
            return turned[pl.ds(256 * k, 256), :]

        one, two = 0, 1
        push(weights(*order[0], 0), one, True)
        push(turned_block(order[0][1]), two)
        yield None
        for n, (p, k) in enumerate(order):
            lhs = z_ref[:, pl.ds(256 * k, 256)]
            following = order[n + 1] if n + 1 < len(order) else None
            pltpu.matmul_acc_lhs(acc_a[p % 2][0], lhs, load_staged_rhs=one)
            push(weights(p, k, 1), one, True)
            if n and order[n - 1][0] < p:
                yield p - 1
            pltpu.matmul_acc_lhs(acc_b, part(2 * p + 1, HEAD_ROWS * (k // 3), HEAD_ROWS, k % 3), load_staged_rhs=two)
            if following:
                need(following[0])
                push(weights(*following, 0), two, True)
            pltpu.matmul_acc_lhs(acc_a[p % 2][1], lhs, load_staged_rhs=one)
            if following:
                push(turned_block(following[1]), one)
            one, two = two, one
            yield None
        yield pairs - 1

    def run(*accs):
        acc_a, acc_b = ((accs[0:2], accs[2:4]), (accs[4:6], accs[6:8])), accs[8:]
        for acc in accs:
            pltpu.matmul_pop(acc)
        waited = set()

        def need(p):
            for chunk in (2 * p, 2 * p + 1):
                if chunk >= HEAD_EARLY and chunk not in waited:
                    waited.add(chunk)
                    i = chunk - HEAD_EARLY
                    pltpu.make_async_copy(late.at[i], late.at[i], late_sem.at[i]).wait()

        def write(chunk, value):
            logits_ref[:, pl.ds(chunk * HEAD_ROWS, HEAD_ROWS)] = 30.0 * jnp.tanh(value[:4] / 30.0)

        running = {q: unit(q, acc_a[q], acc_b[q], need) for q in range(2)}
        half_done = {}
        while running:
            for q in list(running):
                p = next(running[q], "end")
                if p == "end":
                    del running[q]
                elif p is not None:
                    popped = [pltpu.matmul_pop(acc_b[q])[:, :128]] + [pltpu.matmul_pop(acc) for acc in acc_a[q][p % 2]]
                    if p not in half_done:
                        half_done[p] = popped
                        continue
                    tall, left, right = [x + y for x, y in zip(popped, half_done.pop(p))]
                    write(2 * p, jnp.concatenate([left, right], axis=1))
                    write(2 * p + 1, jnp.concatenate([tall[128 * t:128 * (t + 1)].T[:8] for t in range(4)], axis=1))

    pl.run_scoped(run, *[pltpu.ACC(q)((16, 256), F32) for q in (0, 0, 0, 0, 1, 1, 1, 1)],
                  *[pltpu.ACC(q)((HEAD_ROWS, 256), F32) for q in (0, 1)])
    final = pltpu.make_async_copy(logits_ref, logits_out, out_sem.at[2])
    final.start()
    for copy in keep + [final]:
        copy.wait()


def device_step(tokens, lengths, table, gains, wq, wk, wv, wo, wg, wu, wd, kl, vl, kg, vg):
    vocab_local = table.shape[0]
    vmem, hbm = pl.BlockSpec(memory_space=pltpu.VMEM), pl.BlockSpec(memory_space=pl.ANY)
    smem = pl.BlockSpec(memory_space=pltpu.SMEM)
    emb = pl.pallas_call(
        embed_kernel,
        out_shape=pltpu.VMEM((PIECES, 8, 384), BF16),
        in_specs=[smem, hbm],
        out_specs=vmem,
        scratch_shapes=[pltpu.VMEM((4, 8, DIM), BF16), pltpu.SemaphoreType.DMA((4,))],
    )(tokens, table)
    freq = jnp.asarray((10000.0 ** (-2.0 * np.arange(128, dtype=np.float64) / 256)).astype(np.float32)[None])

    def in_vmem(value):
        return pltpu.with_memory_space_constraint(value, pltpu.VMEM)

    def flat(cache):
        return cache.transpose(0, 2, 1, 3).reshape(4, cache.shape[1], 256)

    results = (jax.ShapeDtypeStruct((4, vocab_local), F32), jax.ShapeDtypeStruct((2, 4, 256), BF16), jax.ShapeDtypeStruct((2, 4, 256), BF16))
    z, nk, nv, ring = pl.pallas_call(
        step_kernel,
        out_shape=(pltpu.VMEM((16, DIM), BF16),) + tuple(pltpu.VMEM(r.shape, r.dtype) for r in results[1:]) + (pltpu.VMEM((RING, 2560, PIECE), BF16),),
        in_specs=[smem, vmem] + [hbm] * 14,
        out_specs=(vmem,) * 4,
        scratch_shapes=[
            pltpu.VMEM((CACHE, 4096, 256), BF16),
            pltpu.VMEM((5, N_DEV, PIECES, 8, 384), BF16),
            pltpu.VMEM((9, DIM), BF16),
            pltpu.VMEM((1, 128), F32),
            pltpu.SemaphoreType.DMA((RING,)),
            pltpu.SemaphoreType.DMA((CACHE,)),
            pltpu.SemaphoreType.DMA((5,)),
            pltpu.SemaphoreType.DMA((5,)),
            pltpu.SemaphoreType.DMA((2,)),
        ],
        compiler_params=pltpu.CompilerParams(collective_id=0, has_side_effects=True, vmem_limit_bytes=25_000_000),
    )(lengths, in_vmem(emb), gains, freq, wq, wk, wv, wo, wg, wu, wd, table,
      flat(kl).reshape(-1, 256), flat(vl).reshape(-1, 256), flat(kg), flat(vg))
    late = vocab_local // HEAD_ROWS - HEAD_EARLY
    return pl.pallas_call(
        head_kernel,
        out_shape=results,
        in_specs=[vmem] * 4 + [hbm],
        out_specs=(hbm,) * 3,
        scratch_shapes=[
            pltpu.VMEM((late, 2560, PIECE), BF16),
            pltpu.VMEM((DIM, 256), BF16),
            pltpu.VMEM((4, vocab_local), F32),
            pltpu.SemaphoreType.DMA((late,)),
            pltpu.SemaphoreType.DMA((3,)),
        ],
        compiler_params=pltpu.CompilerParams(vmem_limit_bytes=27_000_000),
    )(in_vmem(z), in_vmem(ring), in_vmem(nk), in_vmem(nv), table)


def solution(mesh):
    cache_spec = P("dp", None, "tp", None)
    col_spec = P(None, None, "tp")
    row_spec = P(None, "tp", None)
    rows_spec = P(None, "dp", "tp")
    in_specs = (P("dp"), P("dp"), P("tp", None), P(), col_spec, col_spec, col_spec, row_spec, col_spec, col_spec, row_spec,
                cache_spec, cache_spec, cache_spec, cache_spec)
    out_specs = (P("dp", "tp"), rows_spec, rows_spec)
    return jax.shard_map(device_step, mesh=mesh, in_specs=in_specs, out_specs=out_specs, check_vma=False)
```

```python
import functools
import math

import jax
import jax.numpy as jnp
import numpy as np
from jax import lax
from jax.experimental import pallas as pl
from jax.experimental.pallas import tpu as pltpu
from jax.sharding import PartitionSpec as P

MESH = pl.DeviceIdType.MESH
F32, BF16 = jnp.float32, jnp.bfloat16
DIM = 3840
N_DEV = 8
RING = 10
CACHE = 10
PIECE = 768
PIECES = 5
HEAD_ROWS = 512
HEAD_EARLY = 6
PER_LAYER = 16
FF_ROWS = (1024, 1024, 1024, 768)


def dot(a, b):
    return jnp.dot(a, b, preferred_element_type=F32)


def dot_t(a, b):
    return lax.dot_general(a, b, (((1,), (1,)), ((), ())), preferred_element_type=F32)


def round_bf16(v):
    return v.astype(BF16).astype(F32)


def step_kernel(len_ref, emb_ref, gains_ref, freq_ref, wq, wk, wv, wo, wg, wu, wd, table, kl, vl, kg, vg,
                z_out, nk_ref, nv_ref, ring,
                cbuf, recv, gain_buf, freq_buf, ring_sem, c_sem, send_sem, recv_sem, small_sem):
    me = lax.axis_index("tp")

    def col_copies(slot, src_a, src_b, off_b, base, width):
        sem = ring_sem.at[slot]
        copies = []
        if src_b is None:
            copies.append((src_a.at[pl.ds(0, 2560), pl.ds(base, width)], ring.at[slot, pl.ds(0, 2560), pl.ds(0, width)]))
            src_b, off_b = src_a, base + 256
        else:
            copies.append((src_a.at[pl.ds(0, 2560), pl.ds(base, 256)], ring.at[slot, pl.ds(0, 2560), pl.ds(0, 256)]))
            copies.append((src_b.at[pl.ds(0, 2560), pl.ds(off_b, 256)], ring.at[slot, pl.ds(0, 2560), pl.ds(256, 256)]))
        copies.append((src_a.at[pl.ds(2560, 1280), pl.ds(base, 256)], ring.at[slot, pl.ds(0, 1280), pl.ds(512, 256)]))
        copies.append((src_b.at[pl.ds(2560, 1280), pl.ds(off_b, width - 256)], ring.at[slot, pl.ds(1280, 1280), pl.ds(512, width - 256)]))
        for src, dst in copies:
            pltpu.make_async_copy(src, dst, sem).start()

    def row_copies(slot, src, row0, rows):
        for j in range(PIECES):
            pltpu.make_async_copy(src.at[pl.ds(row0, rows), pl.ds(PIECE * j, PIECE)],
                                  ring.at[slot, pl.ds(rows * j, rows)], ring_sem.at[slot]).start()

    def issue(i):
        if i >= 2 * PER_LAYER + HEAD_EARLY:
            return
        slot = i % RING
        if i >= 2 * PER_LAYER:
            row_copies(slot, table, (i - 2 * PER_LAYER) * HEAD_ROWS, HEAD_ROWS)
            return
        layer, c = divmod(i, PER_LAYER)
        if c == 0:
            col_copies(slot, wq.at[layer], None, 0, 0, 512)
        elif c == 1:
            col_copies(slot, wk.at[layer], wv.at[layer], 0, 0, 512)
        elif c == 2:
            row_copies(slot, wo.at[layer], 0, 512)
        elif c < 11:
            block, which = divmod(c - 3, 2)
            src, rows, row0 = (wg, wu)[which].at[layer], FF_ROWS[block], 1024 * block
            half = rows // 2
            for src_row, count, col, width, row, at in ((0, rows, 0, PIECE, 0, 0), (0, rows, PIECE, PIECE, rows, 0),
                                                        (0, half, 2 * PIECE, 384, 2 * rows, 0), (half, half, 2 * PIECE, 384, 2 * rows, 384)):
                pltpu.make_async_copy(src.at[pl.ds(row0 + src_row, count), pl.ds(col, width)],
                                      ring.at[slot, pl.ds(row, count), pl.ds(at, width)], ring_sem.at[slot]).start()
        else:
            pltpu.make_async_copy(wd.at[layer, :, pl.ds(PIECE * (c - 11), PIECE)],
                                  ring.at[slot, pl.ds(0, 1920)], ring_sem.at[slot]).start()

    def arrive(i, rows=2560):
        slot = i % RING
        part = ring.at[slot] if rows == 2560 else ring.at[slot, pl.ds(0, rows)]
        pltpu.make_async_copy(part, part, ring_sem.at[slot]).wait()
        return slot

    cache_list = [kl, vl] + [kg.at[b] for b in range(4)] + [vg.at[b] for b in range(4)]

    def issue_cache(i):
        pltpu.make_async_copy(cache_list[i], cbuf.at[i], c_sem.at[i]).start()

    def arrive_cache(i):
        pltpu.make_async_copy(cache_list[i], cbuf.at[i], c_sem.at[i]).wait()
        return i

    core, x_pos, y_pos = lax.rem(me, 2), lax.rem(me // 2, 2), me // 4
    far = [(1 - y_pos, 1 - x_pos, core), (1 - y_pos, 1 - x_pos, 1 - core)]
    near = [(y_pos, 1 - x_pos, core), (1 - y_pos, x_pos, core), (y_pos, 1 - x_pos, 1 - core), (1 - y_pos, x_pos, 1 - core)]
    peers = [(py * 2 + px) * 2 + pc for py, px, pc in far + near + [(y_pos, x_pos, 1 - core)]]

    barrier = pltpu.get_barrier_semaphore()
    for peer in peers:
        pl.semaphore_signal(barrier, inc=1, device_id={"tp": peer}, device_id_type=MESH)

    def start(chunks, caches=()):
        @pl.when(me >= 0)
        def _():
            for i in chunks:
                issue(i)
            for i in caches:
                issue_cache(i)

    gain_copy = pltpu.make_async_copy(gains_ref, gain_buf, small_sem.at[1])
    freq_copy = pltpu.make_async_copy(freq_ref, freq_buf, small_sem.at[0])
    start((0,))
    gain_copy.start()
    freq_copy.start()
    start((1,), (0, 1))
    recv[0, me] = emb_ref[...]
    pl.semaphore_wait(barrier, N_DEV - 1)

    def send(step, piece=None):
        block = recv.at[step, me] if piece is None else recv.at[step, me, piece]
        for peer in peers:
            pltpu.make_async_remote_copy(src_ref=block, dst_ref=block, send_sem=send_sem.at[step], recv_sem=recv_sem.at[step],
                                         device_id={"tp": peer}, device_id_type=MESH).start()

    row = lax.broadcasted_iota(jnp.int32, (8, 128), 0)
    low_rows = row < 4
    req = jnp.where(low_rows, row, row - 4)

    def tile_to(mask, width):
        return jnp.concatenate([mask] * (width // 128), axis=1) if width > 128 else mask

    low_384 = lax.broadcasted_iota(jnp.int32, (8, 384), 0) < 4
    low_256 = lax.broadcasted_iota(jnp.int32, (8, 256), 0) < 4

    def pack(value):
        return jnp.where(low_384, value[:, :384], value[:, 384:]).astype(BF16)

    def collect(step):
        whole = recv.at[step, pl.ds(0, N_DEV - 1)]
        pltpu.make_async_copy(whole, whole, recv_sem.at[step]).wait()
        parts = []
        for piece in range(PIECES):
            total = recv[step, 0, piece].astype(F32)
            for dev in range(1, N_DEV):
                total = total + recv[step, dev, piece].astype(F32)
            total = round_bf16(total)
            other = pltpu.roll(total, 4, 0)
            parts += [jnp.where(low_384, total, other), jnp.where(low_384, other, total)]
        return jnp.concatenate(parts, axis=1)

    send(0)
    for i in range(2, RING):
        start((i,))
    gain_copy.wait()
    freq_copy.wait()

    len_row = jnp.full((8, 128), len_ref[3], jnp.int32)
    for b in range(3):
        len_row = jnp.where(req == b, len_ref[b], len_row)
    angle = len_row.astype(F32) * freq_buf[...]
    cos_tab, sin_tab = jnp.cos(angle), jnp.sin(angle)
    len_col = len_row[:, :1]

    def rotate(head):
        lo, hi = head[:, :128], head[:, 128:]
        return jnp.concatenate([lo * cos_tab - hi * sin_tab, hi * cos_tab + lo * sin_tab], axis=1)

    def norm(value, index):
        gain = gain_buf[pl.ds(index, 1), :].astype(F32)
        inv = lax.rsqrt(jnp.mean(value * value, axis=-1, keepdims=True) + 1e-6)
        return (value * inv * (1.0 + gain)).astype(BF16)

    def dot_cols(x, slot, width):
        head, tail = x[:, :2560], x[:, 2560:]
        main = dot(head, ring[slot, :, pl.ds(0, width)])
        left = dot(tail, ring[slot, pl.ds(0, 1280), pl.ds(512, 256)])
        right = dot(tail, ring[slot, pl.ds(1280, 1280), pl.ds(512, width - 256)])
        return main + jnp.concatenate([left, right], axis=1)

    def dot_rows(x, slot, rows):
        half = rows // 2
        parts = []
        for row in (0, rows):
            parts.append(dot(x, ring[slot, pl.ds(row, rows), pl.ds(0, 512)]))
            parts.append(dot(x, ring[slot, pl.ds(row, rows), pl.ds(512, 256)]))
        top, low = dot(x[:, :half], ring[slot, pl.ds(2 * rows, half), pl.ds(0, 384)]), dot(x[:, half:], ring[slot, pl.ds(2 * rows, half), pl.ds(384, 384)])
        parts.append(top + low)
        return parts

    def dot_piece(x, slot, row0, rows):
        half = 256 * ((rows + 256) // 512)
        left = dot(x, ring[slot, pl.ds(row0, rows), pl.ds(0, 512)])
        one = dot(x[:, :half], ring[slot, pl.ds(row0, half), pl.ds(512, 256)])
        two = dot(-x[:, half:], ring[slot, pl.ds(row0 + half, rows - half), pl.ds(512, 256)])
        return jnp.concatenate([left, one - two], axis=1)

    def cap(scores):
        return 50.0 * jnp.tanh(scores / 50.0)

    def finish_attention(q8, scores, new_k, slots, is_local):
        slot_id = lax.broadcasted_iota(jnp.int32, (8, slots), 1)
        valid = slot_id <= len_col
        write = len_col
        if is_local:
            valid = valid | (len_col >= slots - 1)
            write = lax.rem(len_col, slots)
        valid = valid & (slot_id != write)
        capped = jnp.where(valid, cap(scores), -1e30)
        own = cap(jnp.sum(q8.astype(F32) * new_k.astype(F32), axis=-1, keepdims=True))
        top = jnp.maximum(jnp.max(capped, axis=-1, keepdims=True), own)
        grown, own = jnp.exp(capped - top), jnp.exp(own - top)
        total = jnp.sum(grown, axis=-1, keepdims=True) + own
        return (grown / total).astype(BF16), round_bf16(own / total)

    def layer_step(layer, x, is_local):
        base = PER_LAYER * layer
        a = norm(x, 4 * layer)
        slot = arrive(base)
        q = round_bf16(dot_cols(a, slot, 512))
        slot = arrive(base + 1)
        kv = dot_cols(a, slot, 512).astype(BF16)
        start((base + RING, base + 1 + RING))
        new_k = rotate(kv[:, :256].astype(F32)).astype(BF16)
        new_v = kv[:, 256:]
        nk_ref[layer] = new_k[:4]
        nv_ref[layer] = new_v[:4]
        q_both = jnp.where(low_256, q[:, :256], q[:, 256:])
        q8 = (rotate(q_both) * 0.0625).astype(BF16)

        if is_local:
            slots = 1024
            every = dot_t(q8, cbuf[arrive_cache(0)])
            req_wide = tile_to(req, slots)
            scores = every[:, 3 * slots:]
            for b in range(3):
                scores = jnp.where(req_wide == b, every[:, b * slots:(b + 1) * slots], scores)
        else:
            slots = 4096
            req_wide = tile_to(req, slots)
            scores = None
            for b in range(4):
                one = dot_t(q8, cbuf[arrive_cache(2 + b)])
                scores = one if scores is None else jnp.where(req_wide == b, one, scores)
        probs, own = finish_attention(q8, scores, new_k, slots, is_local)
        mixed = None
        for b in range(4):
            if is_local:
                if b == 0:
                    at = arrive_cache(1)
                one = dot(probs, cbuf[at, pl.ds(b * slots, slots)])
            else:
                at = arrive_cache(6 + b)
                one = dot(probs[:, :2048], cbuf[at, pl.ds(0, 2048)]) - dot(-probs[:, 2048:], cbuf[at, pl.ds(2048, 2048)])
            mixed = one if mixed is None else jnp.where(tile_to(req, 256) == b, one, mixed)
        mixed = round_bf16(mixed + own * new_v.astype(F32))
        other = pltpu.roll(mixed, 4, 0)
        mixed = jnp.concatenate([jnp.where(low_256, mixed, other), jnp.where(low_256, other, mixed)], axis=1).astype(BF16)

        step = 1 + 2 * layer
        slot = arrive(base + 2)
        for j in range(PIECES):
            recv[step, me, j] = pack(dot_piece(mixed, slot, 512 * j, 512))
            send(step, j)
        start((base + 2 + RING,))
        x = round_bf16(x + norm(collect(step), 4 * layer + 1).astype(F32))

        a = norm(x, 4 * layer + 2)
        gate = up = None
        for block, rows in enumerate(FF_ROWS):
            at, filled = base + 3 + 2 * block, 2560 * rows // 1024
            gate_slot, up_slot = arrive(at, filled), arrive(at + 1, filled)
            part = a[:, 1024 * block:1024 * block + rows]
            part = part if block == 0 else -part
            gate_part, up_part = dot_rows(part, gate_slot, rows), dot_rows(part, up_slot, rows)
            gate = gate_part if gate is None else [x - y for x, y in zip(gate, gate_part)]
            up = up_part if up is None else [x - y for x, y in zip(up, up_part)]
            start((at + RING, at + 1 + RING), (2 + 2 * block, 3 + 2 * block) if is_local else ())
        act = jnp.concatenate([(jax.nn.gelu(round_bf16(x), approximate=True) * round_bf16(y)).astype(BF16) for x, y in zip(gate, up)], axis=1)
        step = 2 + 2 * layer
        for j in range(PIECES):
            at = base + 11 + j
            slot = arrive(at, 1920)
            recv[step, me, j] = pack(dot_piece(act, slot, 0, 1920))
            send(step, j)
            start((at + RING,))
        return round_bf16(x + norm(collect(step), 4 * layer + 3).astype(F32))

    x = collect(0)
    x = layer_step(0, x, True)
    x = layer_step(1, x, False)
    z = norm(x, 8)
    z_out[...] = jnp.concatenate([z, z], axis=0)
    for i in range(HEAD_EARLY):
        arrive(2 * PER_LAYER + i)

    for step in range(5):
        whole = recv.at[step, pl.ds(0, N_DEV - 1)]
        pltpu.make_async_copy(whole, whole, send_sem.at[step]).wait()


def embed_kernel(token_ref, table, out_ref, block, sem):
    rows = table.shape[0]
    first = lax.axis_index("tp") * rows
    ids, copies = [], []
    for b in range(4):
        local = token_ref[b] - first
        safe = jnp.clip(local, 0, rows - 1)
        base = pl.multiple_of((safe // 8) * 8, 8)
        copy = pltpu.make_async_copy(table.at[pl.ds(base, 8)], block.at[b], sem.at[b])
        copy.start()
        copies.append(copy)
        ids.append(jnp.where((local >= 0) & (local < rows), safe - base, -1))
    row = lax.broadcasted_iota(jnp.int32, (8, DIM), 0)
    scale = float(np.asarray(math.sqrt(DIM), np.float32).astype(BF16))
    full = jnp.zeros((8, DIM), F32)
    for b in range(4):
        copies[b].wait()
        mine = jnp.sum(jnp.where(row == ids[b], block[b].astype(F32), 0.0), axis=0, keepdims=True)
        full = jnp.where((row == b) | (row == b + 4), mine * scale, full)
    low = lax.broadcasted_iota(jnp.int32, (8, 384), 0) < 4
    for j in range(PIECES):
        out_ref[j] = jnp.where(low, full[:, PIECE * j:PIECE * j + 384], full[:, PIECE * j + 384:PIECE * (j + 1)]).astype(BF16)


def head_kernel(z_ref, early, nk_in, nv_in, table, logits_out, nk_out, nv_out, late, turned, logits_ref, late_sem, out_sem):
    chunks = table.shape[0] // HEAD_ROWS
    pairs, depth = chunks // 2, DIM // 256
    for i in range(0, chunks - HEAD_EARLY, 2):
        for j in range(PIECES):
            for n in (i, i + 1):
                pltpu.make_async_copy(table.at[pl.ds((HEAD_EARLY + n) * HEAD_ROWS, HEAD_ROWS), pl.ds(PIECE * j, PIECE)],
                                      late.at[n, pl.ds(HEAD_ROWS * j, HEAD_ROWS)], late_sem.at[i // 2, j]).start()
    keep = [pltpu.make_async_copy(nk_in, nk_out, out_sem.at[0]), pltpu.make_async_copy(nv_in, nv_out, out_sem.at[1])]
    for copy in keep:
        copy.start()

    turned[:, pl.ds(128, 128)] = jnp.zeros((DIM, 128), BF16)
    for j in range(DIM // 128):
        block = jnp.concatenate([z_ref[:, pl.ds(128 * j, 128)].astype(F32), jnp.zeros((112, 128), F32)], axis=0)
        turned[pl.ds(128 * j, 128), pl.ds(0, 128)] = block.T.astype(BF16)

    def part(chunk, row0, rows, c):
        span = pl.ds(row0, rows), pl.ds(256 * c, 256)
        if chunk < HEAD_EARLY:
            return early[(2 * PER_LAYER + chunk) % RING, span[0], span[1]]
        return late[chunk - HEAD_EARLY, span[0], span[1]]

    def unit(q, acc_a, acc_b, need):
        order = [(p, k) for p in range(pairs) for k in range((q + p) % 2, depth, 2)]

        def push(value, register, transpose=False):
            pltpu.matmul_push_rhs(value, staging_register=register, mxu_index=q, transpose=transpose)

        def weights(p, k, half):
            return part(2 * p, HEAD_ROWS * (k // 3) + 256 * half, 256, k % 3)

        def turned_block(k):
            return turned[pl.ds(256 * k, 256), :]

        one, two = 0, 1
        push(weights(*order[0], 0), one, True)
        push(turned_block(order[0][1]), two)
        yield None
        for n, (p, k) in enumerate(order):
            lhs = z_ref[:, pl.ds(256 * k, 256)]
            following = order[n + 1] if n + 1 < len(order) else None
            pltpu.matmul_acc_lhs(acc_a[p % 2][0], lhs, load_staged_rhs=one)
            push(weights(p, k, 1), one, True)
            if n and order[n - 1][0] < p:
                yield p - 1
            pltpu.matmul_acc_lhs(acc_b, part(2 * p + 1, HEAD_ROWS * (k // 3), HEAD_ROWS, k % 3), load_staged_rhs=two)
            if following:
                need(*following)
                push(weights(*following, 0), two, True)
            pltpu.matmul_acc_lhs(acc_a[p % 2][1], lhs, load_staged_rhs=one)
            if following:
                push(turned_block(following[1]), one)
            one, two = two, one
            yield None
        yield pairs - 1

    def run(*accs):
        acc_a, acc_b = ((accs[0:2], accs[2:4]), (accs[4:6], accs[6:8])), accs[8:]
        for acc in accs:
            pltpu.matmul_pop(acc)
        waited = set()

        def need(p, k):
            key = 2 * p - HEAD_EARLY, k // 3
            if key[0] >= 0 and key not in waited:
                waited.add(key)
                both = late.at[key[0], pl.ds(0, 2 * HEAD_ROWS)]
                pltpu.make_async_copy(both, both, late_sem.at[key[0] // 2, key[1]]).wait()

        def write(chunk, value):
            logits_ref[:, pl.ds(chunk * HEAD_ROWS, HEAD_ROWS)] = 30.0 * jnp.tanh(value[:4] / 30.0)

        running = {q: unit(q, acc_a[q], acc_b[q], need) for q in range(2)}
        half_done = {}
        while running:
            for q in list(running):
                p = next(running[q], "end")
                if p == "end":
                    del running[q]
                elif p is not None:
                    popped = [pltpu.matmul_pop(acc_b[q])[:, :128]] + [pltpu.matmul_pop(acc) for acc in acc_a[q][p % 2]]
                    if p not in half_done:
                        half_done[p] = popped
                        continue
                    tall, left, right = [x + y for x, y in zip(popped, half_done.pop(p))]
                    write(2 * p, jnp.concatenate([left, right], axis=1))
                    write(2 * p + 1, jnp.concatenate([tall[128 * t:128 * (t + 1)].T[:8] for t in range(4)], axis=1))

    pl.run_scoped(run, *[pltpu.ACC(q)((16, 256), F32) for q in (0, 0, 0, 0, 1, 1, 1, 1)],
                  *[pltpu.ACC(q)((HEAD_ROWS, 256), F32) for q in (0, 1)])
    final = pltpu.make_async_copy(logits_ref, logits_out, out_sem.at[2])
    final.start()
    for copy in keep + [final]:
        copy.wait()


def device_step(tokens, lengths, table, gains, wq, wk, wv, wo, wg, wu, wd, kl, vl, kg, vg):
    vocab_local = table.shape[0]
    vmem, hbm = pl.BlockSpec(memory_space=pltpu.VMEM), pl.BlockSpec(memory_space=pl.ANY)
    smem = pl.BlockSpec(memory_space=pltpu.SMEM)
    emb = pl.pallas_call(
        embed_kernel,
        out_shape=pltpu.VMEM((PIECES, 8, 384), BF16),
        in_specs=[smem, hbm],
        out_specs=vmem,
        scratch_shapes=[pltpu.VMEM((4, 8, DIM), BF16), pltpu.SemaphoreType.DMA((4,))],
    )(tokens, table)
    freq = jnp.asarray((10000.0 ** (-2.0 * np.arange(128, dtype=np.float64) / 256)).astype(np.float32)[None])

    def in_vmem(value):
        return pltpu.with_memory_space_constraint(value, pltpu.VMEM)

    def flat(cache):
        return cache.transpose(0, 2, 1, 3).reshape(4, cache.shape[1], 256)

    results = (jax.ShapeDtypeStruct((4, vocab_local), F32), jax.ShapeDtypeStruct((2, 4, 256), BF16), jax.ShapeDtypeStruct((2, 4, 256), BF16))
    z, nk, nv, ring = pl.pallas_call(
        step_kernel,
        out_shape=(pltpu.VMEM((16, DIM), BF16),) + tuple(pltpu.VMEM(r.shape, r.dtype) for r in results[1:]) + (pltpu.VMEM((RING, 2560, PIECE), BF16),),
        in_specs=[smem, vmem] + [hbm] * 14,
        out_specs=(vmem,) * 4,
        scratch_shapes=[
            pltpu.VMEM((CACHE, 4096, 256), BF16),
            pltpu.VMEM((5, N_DEV, PIECES, 8, 384), BF16),
            pltpu.VMEM((9, DIM), BF16),
            pltpu.VMEM((1, 128), F32),
            pltpu.SemaphoreType.DMA((RING,)),
            pltpu.SemaphoreType.DMA((CACHE,)),
            pltpu.SemaphoreType.DMA((5,)),
            pltpu.SemaphoreType.DMA((5,)),
            pltpu.SemaphoreType.DMA((2,)),
        ],
        compiler_params=pltpu.CompilerParams(collective_id=0, has_side_effects=True, vmem_limit_bytes=26_000_000),
    )(lengths, in_vmem(emb), gains, freq, wq, wk, wv, wo, wg, wu, wd, table,
      flat(kl).reshape(-1, 256), flat(vl).reshape(-1, 256), flat(kg), flat(vg))
    late = vocab_local // HEAD_ROWS - HEAD_EARLY
    return pl.pallas_call(
        head_kernel,
        out_shape=results,
        in_specs=[vmem] * 4 + [hbm],
        out_specs=(hbm,) * 3,
        scratch_shapes=[
            pltpu.VMEM((late, 2560, PIECE), BF16),
            pltpu.VMEM((DIM, 256), BF16),
            pltpu.VMEM((4, vocab_local), F32),
            pltpu.SemaphoreType.DMA((late // 2, PIECES)),
            pltpu.SemaphoreType.DMA((3,)),
        ],
        compiler_params=pltpu.CompilerParams(vmem_limit_bytes=27_000_000),
    )(in_vmem(z), in_vmem(ring), in_vmem(nk), in_vmem(nv), table)


def solution(mesh):
    cache_spec = P("dp", None, "tp", None)
    col_spec = P(None, None, "tp")
    row_spec = P(None, "tp", None)
    rows_spec = P(None, "dp", "tp")
    in_specs = (P("dp"), P("dp"), P("tp", None), P(), col_spec, col_spec, col_spec, row_spec, col_spec, col_spec, row_spec,
                cache_spec, cache_spec, cache_spec, cache_spec)
    out_specs = (P("dp", "tp"), rows_spec, rows_spec)
    return jax.shard_map(device_step, mesh=mesh, in_specs=in_specs, out_specs=out_specs, check_vma=False)
```
